32 devices in a mesh: dp: 4 (over x, y), tp: 8 (over z, core).
Axes of the slice: x: 2, y: 2, z: 4, core: 2. Of those that a mesh axis runs over, the one named last changes fastest.
Arguments:
- resid_in: bfloat16 [2048, 1024], P('dp'), parts along dimension 0
- cand_ids: int32 [2048, 256], P('dp'), parts along dimension 0
- ln_mlp: bfloat16 [1024], replicated
- wi_gate: bfloat16 [1024, 2816], P(None, 'tp')
- wi_lin: bfloat16 [1024, 2816], P(None, 'tp')
- w_out: bfloat16 [2816, 1024], P('tp')
- ln_final: bfloat16 [1024], replicated
- w_lm: bfloat16 [1024, 250112], P(None, 'tp')
Outputs:
- output 1: float32 [2048, 256], P('dp'), parts along dimension 0
- output 2: float32 [2048], P('dp'), parts along dimension 0
There are 4 independent parts. The reference program is written for one: setup_inputs(seed, part) draws one part's arguments, and reference() takes and returns one part's arrays. A program takes and returns all parts, laid end to end along the dimension named above; an argument that names none is the same for every part.
All inputs are finite; a program needn't handle non-finite values.
Results may differ from the reference program's by a relative error of at most 0.00164813.
Values sent between devices are 32-bit elements.
A program may use at most 1 GiB of HBM per device.

```python
import math
import jax
import jax.numpy as jnp
from jax import lax

BATCH = 512
CANDS = 256
D_MODEL = 1024
D_FF = 2816
VOCAB = 250112

EPS = 1e-6
ROW_BLOCK = min(8, BATCH)
LOW_IDS = VOCAB // 16
LOGIT_STD = math.sqrt(math.log(VOCAB))


def rms_norm(values_in, scale_vec):
    wide = values_in.astype(jnp.float32)
    mean_sq = jnp.mean(wide * wide, axis=-1, keepdims=True)
    return (wide * lax.rsqrt(mean_sq + EPS) * scale_vec.astype(jnp.float32)).astype(jnp.bfloat16)


def draw_cands(cand_key):
    key_pick, key_low, key_any = jax.random.split(cand_key, 3)
    pick_low = jax.random.randint(key_pick, (BATCH, CANDS), 0, 2) == 0
    low_ids = jax.random.randint(key_low, (BATCH, CANDS), 0, LOW_IDS)
    any_ids = jax.random.randint(key_any, (BATCH, CANDS), 0, VOCAB)
    cand_ids = jnp.where(pick_low, low_ids, any_ids)
    cand_ids = cand_ids.at[0, 0].set(0).at[0, CANDS - 1].set(VOCAB - 1)
    return cand_ids.astype(jnp.int32)


def draw_lm(lm_key):
    def one_block(block_idx):
        block = jax.random.normal(jax.random.fold_in(lm_key, block_idx), (128, VOCAB), jnp.float32)
        return (block * (LOGIT_STD / math.sqrt(D_MODEL))).astype(jnp.bfloat16)
    return lax.map(one_block, jnp.arange(D_MODEL // 128)).reshape(D_MODEL, VOCAB)


def setup_inputs(seed: int = 0, part: int = 0) -> dict:
    base_key = jax.random.key(seed)
    key_x, key_cand = jax.random.split(jax.random.fold_in(base_key, part), 2)
    shared = jax.random.split(base_key, 6)
    resid_in = jax.random.normal(key_x, (BATCH, D_MODEL), jnp.float32).astype(jnp.bfloat16)
    ln_mlp = (1.0 + 0.3 * jax.random.normal(shared[0], (D_MODEL,), jnp.float32)).astype(jnp.bfloat16)
    wi_gate = (jax.random.normal(shared[1], (D_MODEL, D_FF), jnp.float32) / math.sqrt(D_MODEL)).astype(jnp.bfloat16)
    wi_lin = (jax.random.normal(shared[2], (D_MODEL, D_FF), jnp.float32) / math.sqrt(D_MODEL)).astype(jnp.bfloat16)
    w_out = (jax.random.normal(shared[3], (D_FF, D_MODEL), jnp.float32) * (1.5 / math.sqrt(D_FF))).astype(jnp.bfloat16)
    ln_final = (1.0 + 0.3 * jax.random.normal(shared[4], (D_MODEL,), jnp.float32)).astype(jnp.bfloat16)
    return {"resid_in": resid_in, "cand_ids": draw_cands(key_cand), "ln_mlp": ln_mlp, "wi_gate": wi_gate, "wi_lin": wi_lin, "w_out": w_out, "ln_final": ln_final, "w_lm": draw_lm(shared[5])}


def reference(resid_in, cand_ids, ln_mlp, wi_gate, wi_lin, w_out, ln_final, w_lm):
    normed = rms_norm(resid_in, ln_mlp)
    act_gate = jnp.dot(normed, wi_gate, preferred_element_type=jnp.float32)
    act_lin = jnp.dot(normed, wi_lin, preferred_element_type=jnp.float32)
    hidden = (jax.nn.gelu(act_gate, approximate=True) * act_lin).astype(jnp.bfloat16)
    mlp_out = jnp.dot(hidden, w_out, preferred_element_type=jnp.float32)
    resid_out = (resid_in.astype(jnp.float32) + mlp_out).astype(jnp.bfloat16)
    final_z = rms_norm(resid_out, ln_final)

    def row_block(block_args):
        z_rows, id_rows = block_args
        logits = jnp.dot(z_rows, w_lm, preferred_element_type=jnp.float32)
        row_max = jnp.max(logits, axis=-1)
        norm_rows = row_max + jnp.log(jnp.sum(jnp.exp(logits - row_max[:, None]), axis=-1))
        picked = jnp.take_along_axis(logits, id_rows, axis=1)
        return picked - norm_rows[:, None], norm_rows

    num_blocks = BATCH // ROW_BLOCK
    log_probs, log_norm = lax.map(row_block, (final_z.reshape(num_blocks, ROW_BLOCK, D_MODEL), cand_ids.reshape(num_blocks, ROW_BLOCK, CANDS)))
    return log_probs.reshape(BATCH, CANDS), log_norm.reshape(BATCH)
```

```python
import functools

import jax
import jax.numpy as jnp
from jax import lax
from jax.experimental import pallas as pl
from jax.experimental.pallas import tpu as pltpu
from jax.sharding import PartitionSpec as P

EPS = 1e-6
TILE = 2048
SLOTS = 3
ROW_GROUP = 8
LANES = 128
f32 = jnp.float32


def rms_norm(values_in, scale_vec):
    wide = values_in.astype(f32)
    mean_sq = jnp.mean(wide * wide, axis=-1, keepdims=True)
    return (wide * lax.rsqrt(mean_sq + EPS) * scale_vec.astype(f32)).astype(jnp.bfloat16)


def dot_t(a, b):
    return lax.dot_general(a, b, (((1,), (1,)), ((), ())), preferred_element_type=f32)


def absorb(logits, ncols, first_chunk, lane, chunk, top, total, picked, valid=None):
    nk = ncols // LANES
    for r in range(0, logits.shape[0], ROW_GROUP):
        rows = pl.ds(r, ROW_GROUP)
        parts = [logits[rows, LANES * k : LANES * (k + 1)] for k in range(nk)]
        for h in range(picked.shape[1] // LANES):
            cols = pl.ds(LANES * h, LANES)
            lanes_h, chunk_h, acc = lane[rows, cols], chunk[rows, cols], picked[rows, cols]
            for k in range(nk):
                got = jnp.take_along_axis(parts[k], lanes_h, axis=1, mode="promise_in_bounds")
                acc = jnp.where(chunk_h == first_chunk + k, got, acc)
            picked[rows, cols] = acc
        if valid is not None:
            col = lax.broadcasted_iota(jnp.int32, (ROW_GROUP, LANES), 1)
            parts = [p if LANES * (k + 1) <= valid else jnp.where(col < valid - LANES * k, p, -jnp.inf) for k, p in enumerate(parts) if LANES * k < valid]
        old = top[rows, :]
        new = functools.reduce(jnp.maximum, parts, old)
        terms = [jnp.exp(p - new) for p in parts]
        while len(terms) > 1:
            terms = [sum(terms[i : i + 2]) for i in range(0, len(terms), 2)]
        total[rows, :] = total[rows, :] * jnp.exp(old - new) + terms[0]
        top[rows, :] = new


def head_kernel(vocab, z, ids, w_hbm, picked, lse, wbuf, wtail, la, lb, lane, chunk, top, total, sems, tail_sem):
    full = vocab // TILE
    left = vocab - full * TILE
    padded = wtail.shape[0]

    def fetch(j, slot):
        return pltpu.make_async_copy(w_hbm.at[pl.ds(pl.multiple_of(j * TILE, TILE), TILE), :], wbuf.at[slot], sems.at[slot])

    for j in range(SLOTS):
        fetch(j, j).start()
    tail = pltpu.make_async_copy(w_hbm.at[pl.ds(full * TILE, left), :], wtail.at[pl.ds(0, left), :], tail_sem)
    tail.start()
    wtail[left:, :] = jnp.zeros((padded - left, wtail.shape[1]), jnp.bfloat16)
    local = ids[...]
    lane[...] = local & (LANES - 1)
    chunk[...] = jnp.where((local < 0) | (local >= vocab), -1, local >> 7)
    picked[...] = jnp.zeros_like(picked)
    top[...] = jnp.full_like(top, -jnp.inf)
    total[...] = jnp.zeros_like(total)

    bufs = (la, lb)
    fold = functools.partial(absorb, lane=lane, chunk=chunk, top=top, total=total, picked=picked)

    def multiply(j, slot, dst):
        fetch(j, slot).wait()
        dst[...] = dot_t(z[...], wbuf[slot])

    multiply(0, 0, la)

    def body(i, _):
        for u in range(2):
            j = 1 + 2 * i + u
            multiply(j, lax.rem(j, SLOTS), bufs[(1 + u) % 2])
            fold(bufs[u % 2], TILE, (j - 1) * (TILE // LANES))

            @pl.when(j - 1 + SLOTS < full)
            def _():
                fetch(j - 1 + SLOTS, lax.rem(j - 1, SLOTS)).start()

        return 0

    steps = (full - 1) // 2
    lax.fori_loop(0, steps, body, 0)
    j = 1 + 2 * steps
    while j < full:
        multiply(j, j % SLOTS, bufs[j % 2])
        fold(bufs[(j - 1) % 2], TILE, (j - 1) * (TILE // LANES))
        j += 1
    tail.wait()
    bufs[j % 2][:, 0:padded] = dot_t(z[...], wtail[...])
    fold(bufs[(j - 1) % 2], TILE, (j - 1) * (TILE // LANES))
    fold(bufs[j % 2], padded, j * (TILE // LANES), valid=left)
    high = jnp.max(top[...], axis=-1, keepdims=True)
    lse[...] = high + jnp.log(jnp.sum(total[...] * jnp.exp(top[...] - high), axis=-1, keepdims=True))


def head(z, local_ids, w_rows):
    rows, depth = z.shape
    cands = local_ids.shape[1]
    vocab = w_rows.shape[0]
    padded = -(-(vocab % TILE) // LANES) * LANES
    vmem = pl.BlockSpec(memory_space=pltpu.VMEM)
    return pl.pallas_call(
        functools.partial(head_kernel, vocab),
        out_shape=(jax.ShapeDtypeStruct((rows, cands), f32), jax.ShapeDtypeStruct((rows, 1), f32)),
        in_specs=[vmem, vmem, pl.BlockSpec(memory_space=pl.ANY)],
        out_specs=(vmem, vmem),
        scratch_shapes=[
            pltpu.VMEM((SLOTS, TILE, depth), jnp.bfloat16),
            pltpu.VMEM((padded, depth), jnp.bfloat16),
            pltpu.VMEM((rows, TILE), f32),
            pltpu.VMEM((rows, TILE), f32),
            pltpu.VMEM((rows, cands), jnp.int32),
            pltpu.VMEM((rows, cands), jnp.int32),
            pltpu.VMEM((rows, LANES), f32),
            pltpu.VMEM((rows, LANES), f32),
            pltpu.SemaphoreType.DMA((SLOTS,)),
            pltpu.SemaphoreType.DMA,
        ],
        compiler_params=pltpu.CompilerParams(vmem_limit_bytes=60 << 20),
        cost_estimate=pl.CostEstimate(flops=2 * rows * depth * vocab, bytes_accessed=2 * vocab * depth, transcendentals=rows * vocab),
        name="head",
    )(z, local_ids, w_rows)


def solution(mesh):
    n = mesh.shape["tp"]

    def local_step(resid_in, cand_ids, ln_mlp, wi_gate, wi_lin, w_out, ln_final, w_lm):
        normed = rms_norm(resid_in, ln_mlp)
        act_gate = jnp.dot(normed, wi_gate, preferred_element_type=f32)
        act_lin = jnp.dot(normed, wi_lin, preferred_element_type=f32)
        hidden = (jax.nn.gelu(act_gate, approximate=True) * act_lin).astype(jnp.bfloat16)
        mlp_out = lax.psum(jnp.dot(hidden, w_out, preferred_element_type=f32), "tp")
        resid_out = (resid_in.astype(f32) + mlp_out).astype(jnp.bfloat16)
        final_z = rms_norm(resid_out, ln_final)
        me = lax.axis_index("tp")
        picked, lse = head(final_z, cand_ids - me * w_lm.shape[1], w_lm.T)
        slots = jnp.where(lax.broadcasted_iota(jnp.int32, (1, n), 1) == me, lse, 0.0)
        both = lax.psum(jnp.concatenate([picked, slots], axis=1), "tp")
        shares = both[:, cand_ids.shape[1] :]
        high = jnp.max(shares, axis=-1, keepdims=True)
        log_norm = high + jnp.log(jnp.sum(jnp.exp(shares - high), axis=-1, keepdims=True))
        return both[:, : cand_ids.shape[1]] - log_norm, log_norm[:, 0]

    in_specs = (P("dp", None), P("dp", None), P(None), P(None, "tp"), P(None, "tp"), P("tp", None), P(None), P(None, "tp"))
    return jax.shard_map(local_step, mesh=mesh, in_specs=in_specs, out_specs=(P("dp", None), P("dp")), check_vma=False)
```

```python
import functools

import jax
import jax.numpy as jnp
from jax import lax
from jax.experimental import pallas as pl
from jax.experimental.pallas import tpu as pltpu
from jax.sharding import PartitionSpec as P

EPS = 1e-6
TILE = 2048
SLOTS = 3
ROW_GROUP = 8
LANES = 128
f32 = jnp.float32


def dot_t(a, b):
    return lax.dot_general(a, b, (((1,), (1,)), ((), ())), preferred_element_type=f32)


def absorb(logits, ncols, first_chunk, lane, chunk, top, total, picked, valid=None):
    nk = ncols // LANES
    for r in range(0, logits.shape[0], ROW_GROUP):
        rows = pl.ds(r, ROW_GROUP)
        parts = [logits[rows, LANES * k : LANES * (k + 1)] for k in range(nk)]
        for h in range(picked.shape[1] // LANES):
            cols = pl.ds(LANES * h, LANES)
            lanes_h, chunk_h, acc = lane[rows, cols], chunk[rows, cols], picked[rows, cols]
            for k in range(nk):
                got = jnp.take_along_axis(parts[k], lanes_h, axis=1, mode="promise_in_bounds")
                acc = jnp.where(chunk_h == first_chunk + k, got, acc)
            picked[rows, cols] = acc
        if valid is not None:
            col = lax.broadcasted_iota(jnp.int32, (ROW_GROUP, LANES), 1)
            parts = [p if LANES * (k + 1) <= valid else jnp.where(col < valid - LANES * k, p, -jnp.inf) for k, p in enumerate(parts) if LANES * k < valid]
        old = top[rows, :]
        new = functools.reduce(jnp.maximum, parts, old)
        terms = [jnp.exp(p - new) for p in parts]
        while len(terms) > 1:
            terms = [sum(terms[i : i + 2]) for i in range(0, len(terms), 2)]
        total[rows, :] = total[rows, :] * jnp.exp(old - new) + terms[0]
        top[rows, :] = new


def head_kernel(vocab, z, ids, w_hbm, picked, lse, wbuf, wtail, la, lb, lane, chunk, top, total, sems, tail_sem):
    full = vocab // TILE
    left = vocab - full * TILE
    padded = wtail.shape[0]

    def fetch(j, slot):
        return pltpu.make_async_copy(w_hbm.at[pl.ds(pl.multiple_of(j * TILE, TILE), TILE), :], wbuf.at[slot], sems.at[slot])

    for j in range(SLOTS):
        fetch(j, j).start()
    tail = pltpu.make_async_copy(w_hbm.at[pl.ds(full * TILE, left), :], wtail.at[pl.ds(0, left), :], tail_sem)
    tail.start()
    wtail[left:, :] = jnp.zeros((padded - left, wtail.shape[1]), jnp.bfloat16)
    local = ids[...]
    lane[...] = local & (LANES - 1)
    chunk[...] = jnp.where((local < 0) | (local >= vocab), -1, local >> 7)
    picked[...] = jnp.zeros_like(picked)
    top[...] = jnp.full_like(top, -jnp.inf)
    total[...] = jnp.zeros_like(total)

    bufs = (la, lb)
    fold = functools.partial(absorb, lane=lane, chunk=chunk, top=top, total=total, picked=picked)

    def multiply(j, slot, dst):
        fetch(j, slot).wait()
        dst[...] = dot_t(z[...], wbuf[slot])

    multiply(0, 0, la)

    def body(i, _):
        for u in range(2):
            j = 1 + 2 * i + u
            multiply(j, lax.rem(j, SLOTS), bufs[(1 + u) % 2])
            fold(bufs[u % 2], TILE, (j - 1) * (TILE // LANES))

            @pl.when(j - 1 + SLOTS < full)
            def _():
                fetch(j - 1 + SLOTS, lax.rem(j - 1, SLOTS)).start()

        return 0

    steps = (full - 1) // 2
    lax.fori_loop(0, steps, body, 0)
    j = 1 + 2 * steps
    while j < full:
        multiply(j, j % SLOTS, bufs[j % 2])
        fold(bufs[(j - 1) % 2], TILE, (j - 1) * (TILE // LANES))
        j += 1
    tail.wait()
    bufs[j % 2][:, 0:padded] = dot_t(z[...], wtail[...])
    fold(bufs[(j - 1) % 2], TILE, (j - 1) * (TILE // LANES))
    fold(bufs[j % 2], padded, j * (TILE // LANES), valid=left)
    high = jnp.max(top[...], axis=-1, keepdims=True)
    value = high + jnp.log(jnp.sum(total[...] * jnp.exp(top[...] - high), axis=-1, keepdims=True))
    lse[...] = jnp.transpose(jnp.broadcast_to(value, top.shape))[0:8, :]


def head(z, local_ids, w_rows):
    rows, depth = z.shape
    cands = local_ids.shape[1]
    vocab = w_rows.shape[0]
    padded = -(-(vocab % TILE) // LANES) * LANES
    vmem = pl.BlockSpec(memory_space=pltpu.VMEM)
    return pl.pallas_call(
        functools.partial(head_kernel, vocab),
        out_shape=(jax.ShapeDtypeStruct((rows, cands), f32), jax.ShapeDtypeStruct((8, rows), f32)),
        in_specs=[vmem, vmem, pl.BlockSpec(memory_space=pl.ANY)],
        out_specs=(vmem, vmem),
        scratch_shapes=[
            pltpu.VMEM((SLOTS, TILE, depth), jnp.bfloat16),
            pltpu.VMEM((padded, depth), jnp.bfloat16),
            pltpu.VMEM((rows, TILE), f32),
            pltpu.VMEM((rows, TILE), f32),
            pltpu.VMEM((rows, cands), jnp.int32),
            pltpu.VMEM((rows, cands), jnp.int32),
            pltpu.VMEM((rows, LANES), f32),
            pltpu.VMEM((rows, LANES), f32),
            pltpu.SemaphoreType.DMA((SLOTS,)),
            pltpu.SemaphoreType.DMA,
        ],
        compiler_params=pltpu.CompilerParams(vmem_limit_bytes=60 << 20),
        cost_estimate=pl.CostEstimate(flops=2 * rows * depth * vocab, bytes_accessed=2 * vocab * depth, transcendentals=rows * vocab),
        name="head",
    )(z, local_ids, w_rows)


def rms(wide, scale_row):
    mean_sq = jnp.mean(wide * wide, axis=-1, keepdims=True)
    return (wide * lax.rsqrt(mean_sq + EPS) * scale_row).astype(jnp.bfloat16)


class Line:
    def __init__(self, src, total, near, edge, mate, own, sems, step, span):
        self.src, self.total, self.near, self.edge, self.mate, self.own = src, total, near, edge, mate, own
        self.send, self.recv = sems
        self.step, self.span = step, span
        self.me = lax.axis_index("tp")
        self.core = lax.rem(self.me, 2)
        chip = lax.div(self.me, 2)
        self.inner = (chip == 1) | (chip == 2)
        self.outer = jnp.logical_not(self.inner)
        self.sib = self.me + 1 - 2 * self.core
        self.pair = jnp.where(lax.rem(chip, 2) == 0, self.me + 2, self.me - 2)
        self.across = jnp.where(chip == 1, self.me + 2, self.me - 2)
        self.chunks = src.shape[0] // (2 * step)

    def rows(self, k, core):
        per = self.span // (2 * self.step)
        start = self.span * (k // per) + (self.span // 2) * core + self.step * (k % per)
        return pl.ds(pl.multiple_of(start, self.step), self.step)

    def slot(self, k):
        return pl.ds(k * self.step, self.step)

    def copy(self, hop, k, src, dst, target):
        return pltpu.make_async_remote_copy(
            src_ref=src, dst_ref=dst, send_sem=self.send.at[hop, k], recv_sem=self.recv.at[hop, k],
            device_id={"tp": target}, device_id_type=pl.DeviceIdType.MESH)

    def swap(self, k):
        return self.copy(0, k, self.src.at[self.rows(k, 1 - self.core)], self.near.at[self.slot(k)], self.sib)

    def inward(self, k):
        return self.copy(1, k, self.own.at[self.slot(k)], self.edge.at[self.slot(k)], self.pair)

    def cross(self, k):
        return self.copy(2, k, self.own.at[self.slot(k)], self.mate.at[self.slot(k)], self.across)

    def outward(self, k):
        return self.copy(3, k, self.total.at[self.rows(k, self.core)], self.total.at[self.rows(k, self.core)], self.pair)

    def share(self, k, core):
        return self.copy(4, k, self.total.at[self.rows(k, core)], self.total.at[self.rows(k, core)], self.sib)

    def mine(self, k):
        self.swap(k).wait_recv()
        return self.src[self.rows(k, self.core), :] + self.near[self.slot(k), :]

    def outer_in(self, k):
        self.own[self.slot(k), :] = self.mine(k)
        self.inward(k).start()

    def inner_in(self, k):
        mine = self.mine(k)
        self.inward(k).wait_recv()
        self.own[self.slot(k), :] = mine + self.edge[self.slot(k), :]
        self.cross(k).start()

    def inner_out(self, k):
        self.cross(k).wait_recv()
        self.total[self.rows(k, self.core), :] = self.own[self.slot(k), :] + self.mate[self.slot(k), :]
        self.outward(k).start()
        self.share(k, self.core).start()

    def outer_out(self, k):
        self.outward(k).wait_recv()
        self.share(k, self.core).start()

    def run(self, after):
        @pl.when(self.outer)
        def _():
            for k in range(self.chunks):
                self.outer_in(k)
            for k in range(self.chunks + 1):
                if k < self.chunks:
                    self.outer_out(k)
                if k >= 1:
                    after(k - 1)

        @pl.when(self.inner)
        def _():
            for k in range(self.chunks + LAG + 1):
                if k < self.chunks:
                    self.inner_in(k)
                if LAG <= k < self.chunks + LAG:
                    self.inner_out(k - LAG)
                if k >= LAG + 1:
                    after(k - LAG - 1)

    def finish(self, k):
        self.share(k, 1 - self.core).wait_recv()

    def drain(self):
        for k in range(self.chunks):
            self.swap(k).wait_send()
            self.share(k, self.core).wait_send()

            @pl.when(self.outer)
            def _():
                self.inward(k).wait_send()

            @pl.when(self.inner)
            def _():
                self.cross(k).wait_send()
                self.outward(k).wait_send()

    def greet(self, barrier):
        for other in (self.sib, self.pair):
            pl.semaphore_signal(barrier, inc=1, device_id={"tp": other}, device_id_type=pl.DeviceIdType.MESH)

        @pl.when(self.inner)
        def _():
            pl.semaphore_signal(barrier, inc=1, device_id={"tp": self.across}, device_id_type=pl.DeviceIdType.MESH)

    def met(self, barrier):
        @pl.when(self.outer)
        def _():
            pl.semaphore_wait(barrier, 2)

        @pl.when(self.inner)
        def _():
            pl.semaphore_wait(barrier, 3)


LAG = 2
MLP_STEP = 32
PICK_STEP = 64


def line_scratch(rows, width, step):
    half = pltpu.VMEM((rows // 2, width), f32)
    sems = pltpu.SemaphoreType.DMA((5, rows // (2 * step)))
    return [half, half, half, half, sems, sems]


def mlp_kernel(x, scales, gate, lin, out, z, part, total, near, edge, mate, own, send, recv):
    line = Line(part, total, near, edge, mate, own, (send, recv), MLP_STEP, part.shape[0] // 2)
    barrier = pltpu.get_barrier_semaphore()
    line.greet(barrier)
    per = line.chunks // 2
    for h in range(2):
        rows = pl.ds(h * line.span, line.span)
        normed = rms(x[rows, :].astype(f32), scales[0:1, :])
        hidden = (jax.nn.gelu(dot_t(normed, gate[...]), approximate=True) * dot_t(normed, lin[...])).astype(jnp.bfloat16)
        part[rows, :] = jnp.dot(hidden, out[...], preferred_element_type=f32)
        if h == 0:
            line.met(barrier)
        for k in range(per * h, per * (h + 1)):
            line.swap(k).start()

    def normalise(k):
        line.finish(k)
        for core in range(2):
            rows = line.rows(k, core)
            mid = (x[rows, :].astype(f32) + total[rows, :]).astype(jnp.bfloat16)
            z[rows, :] = rms(mid.astype(f32), scales[1:2, :])

    line.run(normalise)
    line.drain()


def mlp(x, scales, gate, lin, out):
    rows, width = x.shape
    vmem = pl.BlockSpec(memory_space=pltpu.VMEM)
    return pl.pallas_call(
        mlp_kernel,
        out_shape=jax.ShapeDtypeStruct(x.shape, jnp.bfloat16),
        in_specs=[vmem] * 5,
        out_specs=vmem,
        scratch_shapes=[pltpu.VMEM((rows, width), f32), pltpu.VMEM((rows, width), f32)] + line_scratch(rows, width, MLP_STEP),
        compiler_params=pltpu.CompilerParams(collective_id=0, has_side_effects=True, vmem_limit_bytes=48 << 20),
        name="mlp",
    )(x, scales, gate, lin, out)


def merge_kernel(n, picked, lse, both, norm, shares, near, edge, mate, own, send, recv, ssend, srecv):
    line = Line(picked, both, near, edge, mate, own, (send, recv), PICK_STEP, picked.shape[0])
    barrier = pltpu.get_barrier_semaphore()
    for d in range(1, n):
        pl.semaphore_signal(barrier, inc=1, device_id={"tp": lax.rem(line.me + d, n)}, device_id_type=pl.DeviceIdType.MESH)
    pl.semaphore_wait(barrier, n - 1)

    def tell(d):
        return pltpu.make_async_remote_copy(
            src_ref=lse, dst_ref=shares.at[line.me], send_sem=ssend.at[d - 1], recv_sem=srecv.at[d - 1],
            device_id={"tp": lax.rem(line.me + d, n)}, device_id_type=pl.DeviceIdType.MESH)

    for k in range(line.chunks):
        line.swap(k).start()
    for d in range(1, n):
        tell(d).start()
    line.run(line.finish)
    for d in range(1, n):
        tell(d).wait_recv()
    shares[line.me] = lse[...]
    high = jnp.max(shares[...], axis=0)
    acc = jnp.sum(jnp.exp(shares[...] - high), axis=0)
    norm[...] = high + jnp.log(acc)
    for d in range(1, n):
        tell(d).wait_send()
    line.drain()


def merge(n, picked, lse):
    rows, cands = picked.shape
    vmem = pl.BlockSpec(memory_space=pltpu.VMEM)
    return pl.pallas_call(
        functools.partial(merge_kernel, n),
        out_shape=(jax.ShapeDtypeStruct(picked.shape, f32), jax.ShapeDtypeStruct(lse.shape, f32)),
        in_specs=[vmem] * 2,
        out_specs=(vmem, vmem),
        scratch_shapes=[pltpu.VMEM((n, *lse.shape), f32)] + line_scratch(rows, cands, PICK_STEP)
        + [pltpu.SemaphoreType.DMA((n - 1,)), pltpu.SemaphoreType.DMA((n - 1,))],
        compiler_params=pltpu.CompilerParams(collective_id=1, has_side_effects=True),
        name="merge",
    )(picked, lse)


def solution(mesh):
    n = mesh.shape["tp"]

    def local_step(resid_in, cand_ids, ln_mlp, wi_gate, wi_lin, w_out, ln_final, w_lm):
        scales = jnp.stack([ln_mlp, ln_final]).astype(f32)
        z = mlp(resid_in, scales, wi_gate.T, wi_lin.T, w_out)
        picked, lse = head(z, cand_ids - lax.axis_index("tp") * w_lm.shape[1], w_lm.T)
        both, norm = merge(n, picked, lse)
        log_norm = norm[0]
        return both - log_norm[:, None], log_norm

    in_specs = (P("dp", None), P("dp", None), P(None), P(None, "tp"), P(None, "tp"), P("tp", None), P(None), P(None, "tp"))
    return jax.shard_map(local_step, mesh=mesh, in_specs=in_specs, out_specs=(P("dp", None), P("dp")), check_vma=False)
```

```python
import functools

import jax
import jax.numpy as jnp
from jax import lax
from jax.experimental import pallas as pl
from jax.experimental.pallas import tpu as pltpu
from jax.sharding import PartitionSpec as P

EPS = 1e-6
TILE = 2048
SLOTS = 3
ROW_GROUP = 8
LANES = 128
f32 = jnp.float32


def dot_t(a, b):
    return lax.dot_general(a, b, (((1,), (1,)), ((), ())), preferred_element_type=f32)


def absorb(logits, ncols, first_chunk, lane, chunk, top, total, picked, valid=None):
    nk = ncols // LANES
    for r in range(0, logits.shape[0], ROW_GROUP):
        rows = pl.ds(r, ROW_GROUP)
        parts = [logits[rows, LANES * k : LANES * (k + 1)] for k in range(nk)]
        for h in range(picked.shape[1] // LANES):
            cols = pl.ds(LANES * h, LANES)
            lanes_h, chunk_h, acc = lane[rows, cols], chunk[rows, cols], picked[rows, cols]
            for k in range(nk):
                got = jnp.take_along_axis(parts[k], lanes_h, axis=1, mode="promise_in_bounds")
                acc = jnp.where(chunk_h == first_chunk + k, got, acc)
            picked[rows, cols] = acc
        if valid is not None:
            col = lax.broadcasted_iota(jnp.int32, (ROW_GROUP, LANES), 1)
            parts = [p if LANES * (k + 1) <= valid else jnp.where(col < valid - LANES * k, p, -jnp.inf) for k, p in enumerate(parts) if LANES * k < valid]
        old = top[rows, :]
        new = functools.reduce(jnp.maximum, parts, old)
        terms = [jnp.exp(p - new) for p in parts]
        while len(terms) > 1:
            terms = [sum(terms[i : i + 2]) for i in range(0, len(terms), 2)]
        total[rows, :] = total[rows, :] * jnp.exp(old - new) + terms[0]
        top[rows, :] = new


def head_kernel(vocab, z_in, ids_in, w_hbm, picked, lse, z, ids, in_sems, wbuf, wtail, la, lb, lane, chunk, top, total, sems, tail_sem):
    full = vocab // TILE
    left = vocab - full * TILE
    padded = wtail.shape[0]

    def fetch(j, slot):
        return pltpu.make_async_copy(w_hbm.at[pl.ds(pl.multiple_of(j * TILE, TILE), TILE), :], wbuf.at[slot], sems.at[slot])

    loads = [pltpu.make_async_copy(z_in, z, in_sems.at[0]), pltpu.make_async_copy(ids_in, ids, in_sems.at[1])]
    for load in loads:
        load.start()
    for j in range(SLOTS):
        fetch(j, j).start()
    tail = pltpu.make_async_copy(w_hbm.at[pl.ds(full * TILE, left), :], wtail.at[pl.ds(0, left), :], tail_sem)
    tail.start()
    wtail[left:, :] = jnp.zeros((padded - left, wtail.shape[1]), jnp.bfloat16)
    for load in loads:
        load.wait()
    local = ids[...] - lax.axis_index("tp") * vocab
    lane[...] = local & (LANES - 1)
    chunk[...] = jnp.where((local < 0) | (local >= vocab), -1, local >> 7)
    picked[...] = jnp.zeros_like(picked)
    top[...] = jnp.full_like(top, -jnp.inf)
    total[...] = jnp.zeros_like(total)

    bufs = (la, lb)
    fold = functools.partial(absorb, lane=lane, chunk=chunk, top=top, total=total, picked=picked)

    def multiply(j, slot, dst):
        fetch(j, slot).wait()
        dst[...] = dot_t(z[...], wbuf[slot])

    multiply(0, 0, la)

    def body(i, _):
        for u in range(2):
            j = 1 + 2 * i + u
            multiply(j, lax.rem(j, SLOTS), bufs[(1 + u) % 2])
            fold(bufs[u % 2], TILE, (j - 1) * (TILE // LANES))

            @pl.when(j - 1 + SLOTS < full)
            def _():
                fetch(j - 1 + SLOTS, lax.rem(j - 1, SLOTS)).start()

        return 0

    steps = (full - 1) // 2
    lax.fori_loop(0, steps, body, 0)
    j = 1 + 2 * steps
    while j < full:
        multiply(j, j % SLOTS, bufs[j % 2])
        fold(bufs[(j - 1) % 2], TILE, (j - 1) * (TILE // LANES))
        j += 1
    tail.wait()
    bufs[j % 2][:, 0:padded] = dot_t(z[...], wtail[...])
    fold(bufs[(j - 1) % 2], TILE, (j - 1) * (TILE // LANES))
    fold(bufs[j % 2], padded, j * (TILE // LANES), valid=left)
    high = jnp.max(top[...], axis=-1, keepdims=True)
    value = high + jnp.log(jnp.sum(total[...] * jnp.exp(top[...] - high), axis=-1, keepdims=True))
    lse[...] = jnp.transpose(jnp.broadcast_to(value, top.shape))[0:8, :]


def head(z, ids, w_rows):
    rows, depth = z.shape
    cands = ids.shape[1]
    vocab = w_rows.shape[0]
    padded = -(-(vocab % TILE) // LANES) * LANES
    vmem = pl.BlockSpec(memory_space=pltpu.VMEM)
    return pl.pallas_call(
        functools.partial(head_kernel, vocab),
        out_shape=(jax.ShapeDtypeStruct((rows, cands), f32), jax.ShapeDtypeStruct((8, rows), f32)),
        in_specs=[pl.BlockSpec(memory_space=pl.ANY)] * 3,
        out_specs=(vmem, vmem),
        scratch_shapes=[
            pltpu.VMEM(z.shape, z.dtype),
            pltpu.VMEM(ids.shape, ids.dtype),
            pltpu.SemaphoreType.DMA((2,)),
            pltpu.VMEM((SLOTS, TILE, depth), jnp.bfloat16),
            pltpu.VMEM((padded, depth), jnp.bfloat16),
            pltpu.VMEM((rows, TILE), f32),
            pltpu.VMEM((rows, TILE), f32),
            pltpu.VMEM((rows, cands), jnp.int32),
            pltpu.VMEM((rows, cands), jnp.int32),
            pltpu.VMEM((rows, LANES), f32),
            pltpu.VMEM((rows, LANES), f32),
            pltpu.SemaphoreType.DMA((SLOTS,)),
            pltpu.SemaphoreType.DMA,
        ],
        compiler_params=pltpu.CompilerParams(vmem_limit_bytes=62 << 20),
        cost_estimate=pl.CostEstimate(flops=2 * rows * depth * vocab, bytes_accessed=2 * vocab * depth, transcendentals=rows * vocab),
        name="head",
    )(z, ids, w_rows)


def rms(wide, scale_row):
    mean_sq = jnp.mean(wide * wide, axis=-1, keepdims=True)
    return (wide * lax.rsqrt(mean_sq + EPS) * scale_row).astype(jnp.bfloat16)


class Line:
    def __init__(self, src, total, near, edge, mate, own, sems, step, span):
        self.src, self.total, self.near, self.edge, self.mate, self.own = src, total, near, edge, mate, own
        self.send, self.recv = sems
        self.step, self.span = step, span
        self.me = lax.axis_index("tp")
        self.core = lax.rem(self.me, 2)
        chip = lax.div(self.me, 2)
        self.inner = (chip == 1) | (chip == 2)
        self.outer = jnp.logical_not(self.inner)
        self.sib = self.me + 1 - 2 * self.core
        self.pair = jnp.where(lax.rem(chip, 2) == 0, self.me + 2, self.me - 2)
        self.across = jnp.where(chip == 1, self.me + 2, self.me - 2)
        self.chunks = src.shape[0] // (2 * step)

    def rows(self, k, core):
        per = self.span // (2 * self.step)
        start = self.span * (k // per) + (self.span // 2) * core + self.step * (k % per)
        return pl.ds(pl.multiple_of(start, self.step), self.step)

    def slot(self, k):
        return pl.ds(k * self.step, self.step)

    def copy(self, hop, k, src, dst, target):
        return pltpu.make_async_remote_copy(
            src_ref=src, dst_ref=dst, send_sem=self.send.at[hop, k], recv_sem=self.recv.at[hop, k],
            device_id={"tp": target}, device_id_type=pl.DeviceIdType.MESH)

    def swap(self, k):
        return self.copy(0, k, self.src.at[self.rows(k, 1 - self.core)], self.near.at[self.slot(k)], self.sib)

    def inward(self, k):
        return self.copy(1, k, self.own.at[self.slot(k)], self.edge.at[self.slot(k)], self.pair)

    def cross(self, k):
        return self.copy(2, k, self.own.at[self.slot(k)], self.mate.at[self.slot(k)], self.across)

    def outward(self, k):
        return self.copy(3, k, self.total.at[self.rows(k, self.core)], self.total.at[self.rows(k, self.core)], self.pair)

    def share(self, k, core):
        return self.copy(4, k, self.total.at[self.rows(k, core)], self.total.at[self.rows(k, core)], self.sib)

    def mine(self, k):
        self.swap(k).wait_recv()
        return self.src[self.rows(k, self.core), :] + self.near[self.slot(k), :]

    def outer_in(self, k):
        self.own[self.slot(k), :] = self.mine(k)
        self.inward(k).start()

    def inner_in(self, k):
        mine = self.mine(k)
        self.inward(k).wait_recv()
        self.own[self.slot(k), :] = mine + self.edge[self.slot(k), :]
        self.cross(k).start()

    def inner_out(self, k):
        self.cross(k).wait_recv()
        self.total[self.rows(k, self.core), :] = self.own[self.slot(k), :] + self.mate[self.slot(k), :]
        self.outward(k).start()
        self.share(k, self.core).start()

    def outer_out(self, k):
        self.outward(k).wait_recv()
        self.share(k, self.core).start()

    def run(self, after):
        @pl.when(self.outer)
        def _():
            for k in range(self.chunks):
                self.outer_in(k)
            for k in range(self.chunks + 1):
                if k < self.chunks:
                    self.outer_out(k)
                if k >= 1:
                    after(k - 1)

        @pl.when(self.inner)
        def _():
            for k in range(self.chunks + LAG + 1):
                if k < self.chunks:
                    self.inner_in(k)
                if LAG <= k < self.chunks + LAG:
                    self.inner_out(k - LAG)
                if k >= LAG + 1:
                    after(k - LAG - 1)

    def finish(self, k):
        self.share(k, 1 - self.core).wait_recv()

    def drain(self):
        for k in range(self.chunks):
            self.swap(k).wait_send()
            self.share(k, self.core).wait_send()

            @pl.when(self.outer)
            def _():
                self.inward(k).wait_send()

            @pl.when(self.inner)
            def _():
                self.cross(k).wait_send()
                self.outward(k).wait_send()

    def greet(self, barrier):
        for other in (self.sib, self.pair):
            pl.semaphore_signal(barrier, inc=1, device_id={"tp": other}, device_id_type=pl.DeviceIdType.MESH)

        @pl.when(self.inner)
        def _():
            pl.semaphore_signal(barrier, inc=1, device_id={"tp": self.across}, device_id_type=pl.DeviceIdType.MESH)

    def met(self, barrier):
        @pl.when(self.outer)
        def _():
            pl.semaphore_wait(barrier, 2)

        @pl.when(self.inner)
        def _():
            pl.semaphore_wait(barrier, 3)


LAG = 3
MLP_STEP = 16
PICK_STEP = 32
MERGE_LAG = 3


def line_scratch(rows, width, step):
    half = pltpu.VMEM((rows // 2, width), f32)
    sems = pltpu.SemaphoreType.DMA((5, rows // (2 * step)))
    return [half, half, half, half, sems, sems]


def mlp_kernel(x_in, scales, gate_in, lin_in, out_in, z, x, gate, lin, out, in_sems, part, total, near, edge, mate, own, send, recv):
    line = Line(part, total, near, edge, mate, own, (send, recv), MLP_STEP, part.shape[0] // 2)
    barrier = pltpu.get_barrier_semaphore()
    line.greet(barrier)
    loads = [pltpu.make_async_copy(src, dst, in_sems.at[i]) for i, (src, dst) in enumerate(
        ((x_in, x), (gate_in, gate), (lin_in, lin), (out_in, out)))]
    for load in loads:
        load.start()
    for load in loads[:3]:
        load.wait()
    per = line.chunks // 2
    for h in range(2):
        rows = pl.ds(h * line.span, line.span)
        normed = rms(x[rows, :].astype(f32), scales[0:1, :])
        hidden = (jax.nn.gelu(dot_t(normed, gate[...]), approximate=True) * dot_t(normed, lin[...])).astype(jnp.bfloat16)
        if h == 0:
            loads[3].wait()
        part[rows, :] = jnp.dot(hidden, out[...], preferred_element_type=f32)
        if h == 0:
            line.met(barrier)
        for k in range(per * h, per * (h + 1)):
            line.swap(k).start()

    def normalise(k):
        line.finish(k)
        for core in range(2):
            rows = line.rows(k, core)
            mid = (x[rows, :].astype(f32) + total[rows, :]).astype(jnp.bfloat16)
            z[rows, :] = rms(mid.astype(f32), scales[1:2, :])

    line.run(normalise)
    line.drain()


def mlp(x, scales, gate, lin, out):
    rows, width = x.shape
    vmem = pl.BlockSpec(memory_space=pltpu.VMEM)
    hbm = pl.BlockSpec(memory_space=pl.ANY)
    return pl.pallas_call(
        mlp_kernel,
        out_shape=jax.ShapeDtypeStruct(x.shape, jnp.bfloat16),
        in_specs=[hbm, vmem, hbm, hbm, hbm],
        out_specs=vmem,
        scratch_shapes=[pltpu.VMEM(a.shape, a.dtype) for a in (x, gate, lin, out)] + [pltpu.SemaphoreType.DMA((4,))]
        + [pltpu.VMEM((rows, width), f32), pltpu.VMEM((rows, width), f32)] + line_scratch(rows, width, MLP_STEP),
        compiler_params=pltpu.CompilerParams(collective_id=0, has_side_effects=True, vmem_limit_bytes=62 << 20),
        name="mlp",
    )(x, scales, gate, lin, out)


class Slots:
    def __init__(self, line, own, recv_buf, sems):
        self.line, self.own, self.buf = line, own, recv_buf
        self.send, self.recv = sems

    def copy(self, hop, src, dst, target):
        return pltpu.make_async_remote_copy(
            src_ref=self.own.at[src], dst_ref=self.buf.at[dst], send_sem=self.send.at[hop], recv_sem=self.recv.at[hop],
            device_id={"tp": target}, device_id_type=pl.DeviceIdType.MESH)

    def hop(self, i):
        line = self.line
        return self.copy(i, i, i, (line.sib, line.pair, line.across, line.pair)[i])

    def begin(self, mine):
        self.own[0, :, :] = mine
        self.hop(0).start()

    def inner_in(self):
        self.hop(0).wait_recv()
        self.hop(1).wait_recv()
        self.own[2, :, :] = self.own[0] + self.buf[0] + self.buf[1]
        self.hop(2).start()

    def inner_out(self):
        self.hop(2).wait_recv()
        self.own[3, :, :] = self.own[2] + self.buf[2]
        self.hop(3).start()

    def outer_in(self):
        self.hop(0).wait_recv()
        self.own[1, :, :] = self.own[0] + self.buf[0]
        self.hop(1).start()

    def outer_out(self):
        self.hop(3).wait_recv()
        self.own[3, :, :] = self.buf[3]

    def drain(self):
        self.hop(0).wait_send()

        @pl.when(self.line.outer)
        def _():
            self.hop(1).wait_send()

        @pl.when(self.line.inner)
        def _():
            self.hop(2).wait_send()
            self.hop(3).wait_send()


def merge_kernel(picked, lse, both, norm, mine, got, ssend, srecv, near, edge, mate, own, send, recv):
    line = Line(picked, both, near, edge, mate, own, (send, recv), PICK_STEP, picked.shape[0])
    slots = Slots(line, mine, got, (ssend, srecv))
    barrier = pltpu.get_barrier_semaphore()
    line.greet(barrier)
    line.met(barrier)
    for k in range(line.chunks):
        line.swap(k).start()
    sub = lax.broadcasted_iota(jnp.int32, lse.shape, 0)
    slots.begin(jnp.where(sub == line.me, lse[...], 0.0))

    @pl.when(line.outer)
    def _():
        for k in range(line.chunks):
            line.outer_in(k)
        slots.outer_in()
        for k in range(line.chunks):
            line.outer_out(k)
        slots.outer_out()

    @pl.when(line.inner)
    def _():
        for k in range(line.chunks + 1):
            if k < line.chunks:
                line.inner_in(k)
            else:
                slots.inner_in()
            if k >= MERGE_LAG:
                line.inner_out(k - MERGE_LAG)
        for k in range(line.chunks + 1 - MERGE_LAG, line.chunks):
            line.inner_out(k)
        slots.inner_out()

    every = mine[3, :, :]
    high = jnp.max(every, axis=0, keepdims=True)
    norm[...] = jnp.broadcast_to(high + jnp.log(jnp.sum(jnp.exp(every - high), axis=0, keepdims=True)), norm.shape)
    for k in range(line.chunks):
        line.finish(k)
    slots.drain()
    line.drain()


def merge(n, picked, lse):
    rows, cands = picked.shape
    vmem = pl.BlockSpec(memory_space=pltpu.VMEM)
    return pl.pallas_call(
        merge_kernel,
        out_shape=(jax.ShapeDtypeStruct(picked.shape, f32), jax.ShapeDtypeStruct(lse.shape, f32)),
        in_specs=[vmem] * 2,
        out_specs=(vmem, vmem),
        scratch_shapes=[pltpu.VMEM((4, *lse.shape), f32), pltpu.VMEM((4, *lse.shape), f32),
                        pltpu.SemaphoreType.DMA((4,)), pltpu.SemaphoreType.DMA((4,))]
        + line_scratch(rows, cands, PICK_STEP),
        compiler_params=pltpu.CompilerParams(collective_id=1, has_side_effects=True),
        name="merge",
    )(picked, lse)


def solution(mesh):
    n = mesh.shape["tp"]

    def local_step(resid_in, cand_ids, ln_mlp, wi_gate, wi_lin, w_out, ln_final, w_lm):
        scales = jnp.stack([ln_mlp, ln_final]).astype(f32)
        z = mlp(resid_in, scales, wi_gate.T, wi_lin.T, w_out)
        picked, lse = head(z, cand_ids, w_lm.T)
        both, norm = merge(n, picked, lse)
        log_norm = norm[0]
        return both - log_norm[:, None], log_norm

    in_specs = (P("dp", None), P("dp", None), P(None), P(None, "tp"), P(None, "tp"), P("tp", None), P(None), P(None, "tp"))
    return jax.shard_map(local_step, mesh=mesh, in_specs=in_specs, out_specs=(P("dp", None), P("dp")), check_vma=False)
```
